32 devices in a mesh: tensor: 4 (over y, x), seq: 8 (over z, core).
Axes of the slice: x: 2, y: 2, z: 4, core: 2. Of those that a mesh axis runs over, the one named last changes fastest.
Arguments:
- key_states: bfloat16 [8, 2, 4096, 1024], P(None, None, 'seq', 'tensor'), may hold values from -6 to 6
- value_states: bfloat16 [8, 2, 4096, 1024], P(None, None, 'seq', 'tensor'), may hold values from -6 to 6
- bin_index: int32 [8, 8, 4096], P(None, 'tensor', 'seq'), may hold values from 0 to 4095
- retain_count: int32 [8], replicated, may hold values from 1 to 4096
Outputs:
- histogram: float32 [8, 8, 2, 4096], P(None, 'tensor', None, 'seq')
- threshold: int32 [8], replicated
The draws below stay inside these ranges and needn't reach their ends.
All inputs are finite; a program needn't handle non-finite values.
Results may differ from the reference program's by a relative error of at most 0.0029.
Values sent between devices are 32-bit elements; how exact they have to be, the bound alone decides.
A program may use at most 64 MiB of HBM per device.

```python
import jax
import jax.numpy as jnp
from jax import lax

KVH = 8
HD = 128
BINS = 4096
PAIRS = 8
TOK_DEV = 512
TOKENS = 4096


def draw_bin_index(key, part):
    blocks = TOKENS // TOK_DEV
    key_centre = jax.random.fold_in(key, 11)
    key_expo = jax.random.fold_in(key, 12)
    key_first = jax.random.fold_in(key, 13)
    key_second = jax.random.fold_in(key, 14)
    centre = jax.random.randint(key_centre, (PAIRS, KVH, blocks, 1), 0, BINS).astype(jnp.int32)
    expo = jax.random.randint(key_expo, (PAIRS, KVH, blocks, 1), 0, 8).astype(jnp.int32)
    spread = jnp.maximum(BINS // jnp.left_shift(jnp.ones_like(expo), expo), 1)
    first = jax.random.randint(key_first, (PAIRS, KVH, blocks, TOK_DEV), 0, BINS).astype(jnp.int32) % spread
    second = jax.random.randint(key_second, (PAIRS, KVH, blocks, TOK_DEV), 0, BINS).astype(jnp.int32) % spread
    placed = (centre + first + second) % BINS
    return placed.reshape(PAIRS, KVH, TOKENS).astype(jnp.int32)


def draw_retain_count(key, part):
    key_count = jax.random.fold_in(key, 21)
    highest = min(4096, TOKENS * KVH)
    return jax.random.randint(key_count, (PAIRS,), 1, highest + 1).astype(jnp.int32)


def block_scale(stream_key, shape, shards, smallest, largest):
    loudness = 1.0
    for position, blocks in shards:
        heights = jax.random.uniform(jax.random.fold_in(jax.random.fold_in(stream_key, 6), position), (blocks,), jnp.float32, smallest / len(shards), largest / len(shards))
        loudness = loudness * jnp.repeat(jnp.exp(heights), shape[position] // blocks).reshape((-1,) + (1,) * (len(shape) - 1 - position))
    return loudness


def centred(stream_key, extent, scale, bound, cuts=(), held_as=jnp.bfloat16):
    loudness = block_scale(stream_key, extent, cuts, -0.22, 0.18) if cuts else 1.0
    result = jax.random.normal(stream_key, extent, jnp.float32) * scale * loudness
    return jnp.minimum(jnp.maximum(result, -bound), bound).astype(held_as)


def setup_inputs(seed: int = 0) -> dict:
    seeds = jax.random.split(jax.random.key(seed), 5)
    return {
        "key_states": centred(seeds[0], (PAIRS, 2, TOKENS, KVH * HD), 1.0, 6.0, ((2, 8), (3, 4))),
        "value_states": centred(seeds[1], (PAIRS, 2, TOKENS, KVH * HD), 1.0, 6.0, ((2, 8), (3, 4))),
        "bin_index": draw_bin_index(jax.random.fold_in(seeds[4], 71), 0),
        "retain_count": draw_retain_count(jax.random.fold_in(seeds[4], 71), 0),
    }


def similarity(states):
    first = states[0].astype(jnp.float32).reshape(TOKENS, KVH, HD)
    second = states[1].astype(jnp.float32).reshape(TOKENS, KVH, HD)
    inner_sum = lax.optimization_barrier(jnp.sum(first * second, axis=-1))
    first_sq = lax.optimization_barrier(jnp.sum(first * first, axis=-1))
    second_sq = lax.optimization_barrier(jnp.sum(second * second, axis=-1))
    return (inner_sum / jnp.sqrt((first_sq + 1.0) * (second_sq + 1.0))).T

def one_head(weight_pair, bins_row):
    summed = jax.ops.segment_sum(weight_pair.T, bins_row, num_segments=BINS)
    counted = jax.ops.segment_sum(jnp.ones_like(weight_pair[0]), bins_row, num_segments=BINS)
    return (summed.T, counted)

def reference(key_states, value_states, bin_index, retain_count):
    key_cos = lax.map(similarity, key_states)
    value_cos = lax.map(similarity, value_states)
    rounded = jnp.stack([key_cos, value_cos], axis=2).astype(jnp.bfloat16)
    rounded = lax.optimization_barrier(rounded)
    weights = rounded.astype(jnp.float32)
    histogram, counts = jax.vmap(jax.vmap(one_head))(weights, bin_index)
    pooled = lax.optimization_barrier(jnp.sum(counts, axis=1))
    cumulative = jnp.cumsum(jnp.cumsum(pooled, axis=0), axis=1)
    target = retain_count.astype(jnp.float32)[:, None]
    threshold = lax.optimization_barrier(jnp.sum((cumulative < target).astype(jnp.int32), axis=1)).astype(jnp.int32)
    return (histogram, threshold)
```

```python
import functools

import jax
import jax.numpy as jnp
from jax import lax
from jax.experimental import pallas as pl
from jax.experimental.pallas import tpu as pltpu
from jax.sharding import PartitionSpec as P

BINS = 4096
LANES = 128
HALF = 64
LAG = 3
EARLY = 1
MESH = pl.DeviceIdType.MESH
NT = (((1,), (1,)), ((), ()))
F32 = jnp.float32
BF16 = jnp.bfloat16


def iota(shape, dim):
    return lax.broadcasted_iota(jnp.int32, shape, dim)


def each(lo, hi, body):
    if hi - lo <= 8:
        for k in range(lo, hi):
            body(k)
    else:

        @pl.loop(lo, hi)
        def _(k):
            body(k)


def flag(cond):
    return jnp.where(cond, jnp.ones((), BF16), jnp.zeros((), BF16))


def narrow(row):
    return row.astype(F32).astype(BF16)


def kernel(
    n, nt, key_hbm, value_hbm, bins_hbm, retain_hbm, out, thresh,
    kv, bins, retain, stage_c, recv_c, mine_t, recv_t, all_g, stage_h, recv_d, comb, recv_h,
    in_sem, bin_sem, cs, cr, ts, tr, gs, gr, ds, dr, hs, hr,
):
    pairs, heads, toks = bins.shape
    width = kv.shape[4] // heads
    lanes = stage_h.shape[4]
    his = BINS // lanes
    per = his // n
    group, chips = 2 * nt, n // 2
    own = pairs // nt
    me = lax.axis_index("seq")
    my_t = lax.axis_index("tensor")
    chip, core = me // 2, me % 2
    spot = my_t * 2 + core

    def in_plane(k):
        g = lax.rem(spot + k, group)
        return {"seq": chip * 2 + g % 2, "tensor": g // 2}

    def in_line(k):
        z = lax.rem(chip + k, chips)
        return z, {"seq": z * 2 + core}

    barrier = pltpu.get_barrier_semaphore()

    def greet(device):
        pl.semaphore_signal(barrier, inc=1, device_id=device, device_id_type=MESH)

    each(1, group, lambda k: greet(in_plane(k)))
    each(1, chips, lambda k: greet(in_line(k)[1]))

    def load(p, i):
        return pltpu.make_async_copy((key_hbm, value_hbm)[i].at[p], kv.at[p, i], in_sem.at[i, p])

    small = (
        pltpu.make_async_copy(bins_hbm, bins, bin_sem.at[0]),
        pltpu.make_async_copy(retain_hbm, retain, bin_sem.at[1]),
    )
    small[0].start()
    for p in range(EARLY):
        load(p, 0).start()
        load(p, 1).start()
    with jax.named_scope("binwait"):
        small[0].wait()
    for p in range(EARLY, pairs):
        load(p, 0).start()
        load(p, 1).start()
    small[1].start()

    shift = HALF.bit_length() - 1
    code = iota((HALF, toks), 0)
    order = narrow(jnp.where(code < HALF // 2, code * 2, code * 2 - HALF + 1))
    code = narrow(code)
    total = jnp.zeros((BINS // LANES, LANES), F32)
    for p in range(pairs):
        grid = None
        for h in range(heads):
            row = bins[p, pl.ds(h, 1), :]
            lo = flag(code == narrow(row & (HALF - 1)))
            hi = flag(order == narrow(row >> shift))
            part = lax.dot_general(hi, lo, NT, preferred_element_type=F32)
            grid = part if grid is None else grid + part
        total += jnp.concatenate([grid[:HALF // 2], grid[HALF // 2:]], axis=1)
        stage_c[p] = total

    with jax.named_scope("barrier"):
        pl.semaphore_wait(barrier, group - 1 + chips - 1)

    def copy_c(p):
        k = lax.rem(p % nt * 2 + 1 - spot + group, group)
        return k, pltpu.make_async_remote_copy(
            src_ref=stage_c.at[p], dst_ref=recv_c.at[p // nt, k], send_sem=cs, recv_sem=cr.at[p // nt],
            device_id={"seq": chip * 2 + 1, "tensor": p % nt}, device_id_type=MESH)

    def got_c(j):
        part = recv_c.at[j, pl.ds(1, group - 1)]
        return pltpu.make_async_copy(part, part, cr.at[j])

    def copy_t(j, k):
        return pltpu.make_async_remote_copy(
            src_ref=mine_t.at[j], dst_ref=recv_t.at[j, k], send_sem=ts, recv_sem=tr.at[j],
            device_id=in_line(k)[1], device_id_type=MESH)

    def got_t(j):
        part = recv_t.at[j, pl.ds(1, chips - 1)]
        return pltpu.make_async_copy(part, part, tr.at[j])

    def copy_g(k):
        return pltpu.make_async_remote_copy(
            src_ref=all_g.at[my_t], dst_ref=all_g.at[my_t], send_sem=gs, recv_sem=gr,
            device_id=in_plane(k), device_id_type=MESH)

    def got_g(m):
        part = all_g.at[pl.ds(0, m)]
        return pltpu.make_async_copy(part, part, gr)

    def copy_d(p):
        return pltpu.make_async_remote_copy(
            src_ref=stage_h.at[p, 1 - core], dst_ref=recv_d.at[p], send_sem=ds, recv_sem=dr.at[p],
            device_id={"seq": chip * 2 + 1 - core}, device_id_type=MESH)

    def copy_h(k, p):
        z, device = in_line(k)
        return pltpu.make_async_remote_copy(
            src_ref=comb.at[z, p], dst_ref=recv_h.at[k, p], send_sem=hs, recv_sem=hr,
            device_id=device, device_id_type=MESH)

    def got_h():
        part = recv_h.at[pl.ds(1, chips - 1)]
        return pltpu.make_async_copy(part, part, hr)

    for p in range(pairs):
        k, copy = copy_c(p)
        pl.when(k > 0)(copy.start)

    blk = LANES
    eye = flag(iota((width, width), 0) == iota((width, width), 1))

    def cosine(p, i, h):
        parts = []
        for t in range(0, toks, blk):
            a = kv[p, i, 0, t:t + blk, h * width:(h + 1) * width]
            b = kv[p, i, 1, t:t + blk, h * width:(h + 1) * width]
            if t // blk in (0, 1, 2, 3):
                a, b = a.T.astype(F32), b.T.astype(F32)
            else:
                both = jnp.concatenate([a, b], axis=0)
                turned = lax.dot_general(eye, both, NT, preferred_element_type=F32)
                a, b = turned[:, :blk], turned[:, blk:]
            ab, aa, bb = (jnp.sum(x, axis=0, keepdims=True) for x in (a * b, a * a, b * b))
            parts.append(ab * lax.rsqrt((aa + 1.0) * (bb + 1.0)))
        return jnp.concatenate(parts, axis=1)

    cut = lanes.bit_length() - 1
    odd = (iota((2 * his, toks), 0) & 1) == 1
    hi_of = narrow(iota((2 * his, toks), 0) >> 1)
    lo_of = narrow(iota((lanes, toks), 0))

    def step(p):
        with jax.named_scope("loadwait"):
            load(p, 0).wait()
            load(p, 1).wait()
        for h in range(heads):
            kc = cosine(p, 0, h)
            vc = cosine(p, 1, h)
            row = bins[p, pl.ds(h, 1), :]
            both = jnp.where(odd, vc, kc).astype(BF16)
            left = jnp.where(hi_of == narrow(row >> cut), both, jnp.zeros_like(both))
            right = flag(lo_of == narrow(row & (lanes - 1)))
            res = lax.dot_general(left, right, NT, preferred_element_type=F32)
            for o in range(n):
                stage_h[p, o % 2, o // 2, pl.ds(h * per * 2, per * 2), :] = res[o * per * 2:(o + 1) * per * 2, :]

    def merge(p):
        with jax.named_scope("waitd"):
            copy_d(p).wait_recv()
        comb[:, p] = stage_h[p, core] + recv_d[p]
        each(1, chips, lambda k: copy_h(k, p).start())

    @pl.loop(0, pairs)
    def _(p):
        step(p)
        copy_d(p).start()

        @pl.when(p >= LAG)
        def _():
            merge(p - LAG)

    for p in range(pairs - LAG, pairs - 1):
        merge(p)

    @pl.when(core == 1)
    def _():
        for j in range(own):
            with jax.named_scope("waitc"):
                got_c(j).wait()
            mine_t[j] = stage_c[j * nt + my_t] + jnp.sum(recv_c[j, 1:group], axis=0)
            each(1, chips, lambda k: copy_t(j, k).start())

    merge(pairs - 1)

    @pl.when(core == 1)
    def _():
        rows = BINS // LANES
        small[1].wait()
        xs = []
        for j in range(own):
            with jax.named_scope("waitt"):
                got_t(j).wait()
            xs.append(mine_t[j] + jnp.sum(recv_t[j, 1:chips], axis=0))
        x = jnp.concatenate(xs, axis=0)
        top = jnp.floor(x * (1.0 / 65536.0))
        x = x - top * 65536.0
        mid = jnp.floor(x * (1.0 / 256.0))
        low = x - mid * 256.0
        digits = [v.astype(BF16) for v in (low, mid, top)]
        size = own * rows
        r0, r1 = iota((size, size), 0), iota((size, size), 1)
        upper = flag(iota((LANES, LANES), 0) <= iota((LANES, LANES), 1))
        before = flag((r0 // rows == r1 // rows) & (r1 < r0))

        def value(parts):
            return parts[0] + parts[1] * 256.0 + parts[2] * 65536.0

        within = value([jnp.dot(v, upper, preferred_element_type=F32) for v in digits])
        ahead = value([jnp.dot(before, v, preferred_element_type=F32) for v in digits])
        cum = within + jnp.sum(ahead, axis=1, keepdims=True)
        for j in range(own):
            goal = retain[j * nt + my_t].astype(F32)
            less = jnp.where(cum[j * rows:(j + 1) * rows] < goal, 1.0, 0.0)
            all_g[my_t, j] = jnp.sum(less, axis=0, keepdims=True)
        each(1, group, lambda k: copy_g(k).start())
        with jax.named_scope("waitg"):
            got_g(nt - 1).wait()

    @pl.when(core == 0)
    def _():
        small[1].wait()
        with jax.named_scope("waitg"):
            got_g(nt).wait()

    counts = jnp.concatenate([all_g[p % nt, p // nt] for p in range(pairs)], axis=0)
    if pairs < LANES:
        counts = jnp.concatenate([counts, jnp.zeros((LANES - pairs, LANES), F32)], axis=0)
    ones = jnp.ones((8, LANES), BF16)
    found = lax.dot_general(ones, counts.astype(BF16), NT, preferred_element_type=F32)
    thresh[...] = found.astype(jnp.int32)

    with jax.named_scope("waith"):
        got_h().wait()
    for p in range(pairs):
        acc = comb[chip, p] + jnp.sum(recv_h[1:chips, p], axis=0)
        for h in range(heads):
            for j in range(per):
                at = (h * per + j) * 2
                out[p, h, :, j * lanes:(j + 1) * lanes] = acc[at:at + 2, :]

    for p in range(pairs):
        k, copy = copy_c(p)
        pl.when(k > 0)(copy.wait_send)

    @pl.when(core == 1)
    def _():
        for j in range(own):
            each(1, chips, lambda k: copy_t(j, k).wait_send())
        each(1, group, lambda k: copy_g(k).wait_send())

    each(0, pairs, lambda p: copy_d(p).wait_send())
    whole = comb.at[pl.ds(0, chips - 1)]
    pltpu.make_async_copy(whole, whole, hs).wait()


def hand_over(hist, thresh, out, threshold):
    out[...] = hist[...]
    threshold[...] = thresh[0, :threshold.shape[0]]


def solution(mesh):
    n, nt = mesh.shape["seq"], mesh.shape["tensor"]

    def per_device(key_states, value_states, bin_index, retain_count):
        pairs, heads, toks = bin_index.shape
        span = BINS // n
        lanes = min(LANES, span)
        per = span // lanes
        group, chips = 2 * nt, n // 2
        own = pairs // nt
        rows = BINS // LANES
        block = (heads * per * 2, lanes)
        vmem = pltpu.VMEM
        dma = pltpu.SemaphoreType.DMA
        args = [
            pltpu.with_memory_space_constraint(x, pltpu.HBM)
            for x in (key_states, value_states, bin_index, retain_count)
        ]
        hist, thresh = pl.pallas_call(
            functools.partial(kernel, n, nt),
            out_shape=(
                jax.ShapeDtypeStruct((pairs, heads, 2, span), F32),
                jax.ShapeDtypeStruct((8, LANES), jnp.int32),
            ),
            in_specs=[pl.BlockSpec(memory_space=pltpu.HBM)] * 4,
            out_specs=(pl.BlockSpec(memory_space=vmem), pl.BlockSpec(memory_space=vmem)),
            scratch_shapes=[
                vmem((pairs, 2) + key_states.shape[1:], BF16),
                vmem(bin_index.shape, jnp.int32),
                pltpu.SMEM(retain_count.shape, jnp.int32),
                vmem((pairs, rows, LANES), F32),
                vmem((own, group, rows, LANES), F32),
                vmem((own, rows, LANES), F32),
                vmem((own, chips, rows, LANES), F32),
                vmem((nt, own, 1, LANES), F32),
                vmem((pairs, 2, chips) + block, F32),
                vmem((pairs, chips) + block, F32),
                vmem((chips, pairs) + block, F32),
                vmem((chips, pairs) + block, F32),
                dma((2, pairs)), dma((2,)),
                dma, dma((own,)), dma, dma((own,)),
                dma, dma, dma, dma((pairs,)),
                dma, dma,
            ],
            compiler_params=pltpu.CompilerParams(
                collective_id=0, has_side_effects=True, vmem_limit_bytes=32 * 2**20
            ),
        )(*args)
        return pl.pallas_call(
            hand_over,
            out_shape=(
                jax.ShapeDtypeStruct(hist.shape, F32),
                jax.ShapeDtypeStruct(retain_count.shape, jnp.int32),
            ),
            in_specs=[pl.BlockSpec(memory_space=vmem)] * 2,
            out_specs=(pl.BlockSpec(memory_space=vmem), pl.BlockSpec(memory_space=vmem)),
            compiler_params=pltpu.CompilerParams(vmem_limit_bytes=4 * 2**20),
        )(hist, thresh)

    in_specs = (
        P(None, None, "seq", "tensor"),
        P(None, None, "seq", "tensor"),
        P(None, "tensor", "seq"),
        P(),
    )
    out_specs = (P(None, "tensor", None, "seq"), P())
    return jax.shard_map(
        per_device, mesh=mesh, in_specs=in_specs, out_specs=out_specs, check_vma=False
    )
```

```python
import functools

import jax
import jax.numpy as jnp
from jax import lax
from jax.experimental import pallas as pl
from jax.experimental.pallas import tpu as pltpu
from jax.sharding import PartitionSpec as P

BINS = 4096
LANES = 128
HALF = 64
LAG = 2
EARLY = 1
TURN = 5
MESH = pl.DeviceIdType.MESH
NT = (((1,), (1,)), ((), ()))
F32 = jnp.float32
BF16 = jnp.bfloat16


def iota(shape, dim):
    return lax.broadcasted_iota(jnp.int32, shape, dim)


def each(lo, hi, body):
    if hi - lo <= 8:
        for k in range(lo, hi):
            body(k)
    else:

        @pl.loop(lo, hi)
        def _(k):
            body(k)


def flag(cond):
    return jnp.where(cond, jnp.ones((), BF16), jnp.zeros((), BF16))


def narrow(row):
    return row.astype(F32).astype(BF16)


def kernel(
    n, nt, key_hbm, value_hbm, bins_hbm, retain_hbm, out, thresh,
    kv, bins, retain, stage_c, recv_c, mine_t, recv_t, all_g, stage_h, recv_d, comb, recv_h,
    in_sem, bin_sem, cs, cr, ts, tr, gs, gr, ds, dr, hs, hr,
):
    pairs, heads, toks = bins.shape
    width = kv.shape[4] // heads
    lanes = stage_h.shape[4]
    his = BINS // lanes
    per = his // n
    group, chips = 2 * nt, n // 2
    own = pairs // nt
    me = lax.axis_index("seq")
    my_t = lax.axis_index("tensor")
    chip, core = me // 2, me % 2
    spot = my_t * 2 + core

    def in_plane(k):
        g = lax.rem(spot + k, group)
        return {"seq": chip * 2 + g % 2, "tensor": g // 2}

    def in_line(k):
        z = lax.rem(chip + k, chips)
        return z, {"seq": z * 2 + core}

    barrier = pltpu.get_barrier_semaphore()

    def greet(device):
        pl.semaphore_signal(barrier, inc=1, device_id=device, device_id_type=MESH)

    each(1, group, lambda k: greet(in_plane(k)))
    each(1, chips, lambda k: greet(in_line(k)[1]))

    def load(p, i):
        return pltpu.make_async_copy((key_hbm, value_hbm)[i].at[p], kv.at[p, i], in_sem.at[i, p])

    small = (
        pltpu.make_async_copy(bins_hbm, bins, bin_sem.at[0]),
        pltpu.make_async_copy(retain_hbm, retain, bin_sem.at[1]),
    )
    small[0].start()
    for p in range(EARLY):
        load(p, 0).start()
        load(p, 1).start()
    with jax.named_scope("binwait"):
        small[0].wait()
    for p in range(EARLY, pairs):
        load(p, 0).start()
        load(p, 1).start()
    small[1].start()

    shift = HALF.bit_length() - 1
    code = iota((HALF, toks), 0)
    order = narrow(jnp.where(code < HALF // 2, code * 2, code * 2 - HALF + 1))
    code = narrow(code)
    total = jnp.zeros((BINS // LANES, LANES), F32)
    for p in range(pairs):
        grid = None
        for h in range(heads):
            row = bins[p, pl.ds(h, 1), :]
            lo = flag(code == narrow(row & (HALF - 1)))
            hi = flag(order == narrow(row >> shift))
            part = lax.dot_general(hi, lo, NT, preferred_element_type=F32)
            grid = part if grid is None else grid + part
        total += jnp.concatenate([grid[:HALF // 2], grid[HALF // 2:]], axis=1)
        stage_c[p] = total

    with jax.named_scope("barrier"):
        pl.semaphore_wait(barrier, group - 1 + chips - 1)

    def copy_c(p):
        k = lax.rem(p % nt * 2 + 1 - spot + group, group)
        return k, pltpu.make_async_remote_copy(
            src_ref=stage_c.at[p], dst_ref=recv_c.at[p // nt, k], send_sem=cs, recv_sem=cr.at[p // nt],
            device_id={"seq": chip * 2 + 1, "tensor": p % nt}, device_id_type=MESH)

    def got_c(j):
        part = recv_c.at[j, pl.ds(1, group - 1)]
        return pltpu.make_async_copy(part, part, cr.at[j])

    def copy_t(j, k):
        return pltpu.make_async_remote_copy(
            src_ref=mine_t.at[j], dst_ref=recv_t.at[j, k], send_sem=ts, recv_sem=tr.at[j],
            device_id=in_line(k)[1], device_id_type=MESH)

    def got_t(j):
        part = recv_t.at[j, pl.ds(1, chips - 1)]
        return pltpu.make_async_copy(part, part, tr.at[j])

    def copy_g(k):
        return pltpu.make_async_remote_copy(
            src_ref=all_g.at[my_t], dst_ref=all_g.at[my_t], send_sem=gs, recv_sem=gr,
            device_id=in_plane(k), device_id_type=MESH)

    def got_g(m):
        part = all_g.at[pl.ds(0, m)]
        return pltpu.make_async_copy(part, part, gr)

    def copy_d(p):
        return pltpu.make_async_remote_copy(
            src_ref=stage_h.at[p, 1 - core], dst_ref=recv_d.at[p], send_sem=ds, recv_sem=dr.at[p],
            device_id={"seq": chip * 2 + 1 - core}, device_id_type=MESH)

    def copy_h(k, p):
        z, device = in_line(k)
        return pltpu.make_async_remote_copy(
            src_ref=comb.at[z, p], dst_ref=recv_h.at[k, p], send_sem=hs, recv_sem=hr,
            device_id=device, device_id_type=MESH)

    def got_h():
        part = recv_h.at[pl.ds(1, chips - 1)]
        return pltpu.make_async_copy(part, part, hr)

    for p in range(pairs):
        k, copy = copy_c(p)
        pl.when(k > 0)(copy.start)

    blk = LANES
    eye = flag(iota((width, width), 0) == iota((width, width), 1))

    def cosine(p, i, h):
        parts = []
        for t in range(0, toks, blk):
            a = kv[p, i, 0, t:t + blk, h * width:(h + 1) * width]
            b = kv[p, i, 1, t:t + blk, h * width:(h + 1) * width]
            if t // blk in (0, 1, 2, 3):
                a, b = a.T.astype(F32), b.T.astype(F32)
            else:
                both = jnp.concatenate([a, b], axis=0)
                turned = lax.dot_general(eye, both, NT, preferred_element_type=F32)
                a, b = turned[:, :blk], turned[:, blk:]
            ab, aa, bb = (jnp.sum(x, axis=0, keepdims=True) for x in (a * b, a * a, b * b))
            parts.append(ab * lax.rsqrt((aa + 1.0) * (bb + 1.0)))
        return jnp.concatenate(parts, axis=1)

    cut = lanes.bit_length() - 1
    odd = (iota((2 * his, toks), 0) & 1) == 1
    hi_of = narrow(iota((2 * his, toks), 0) >> 1)
    lo_of = narrow(iota((lanes, toks), 0))

    def step(p):
        with jax.named_scope("loadwait"):
            load(p, 0).wait()
            load(p, 1).wait()
        for h in range(heads):
            kc = cosine(p, 0, h)
            vc = cosine(p, 1, h)
            row = bins[p, pl.ds(h, 1), :]
            both = jnp.where(odd, vc, kc).astype(BF16)
            left = jnp.where(hi_of == narrow(row >> cut), both, jnp.zeros_like(both))
            right = flag(lo_of == narrow(row & (lanes - 1)))
            res = lax.dot_general(left, right, NT, preferred_element_type=F32)
            for o in range(n):
                stage_h[p, o % 2, o // 2, pl.ds(h * per * 2, per * 2), :] = res[o * per * 2:(o + 1) * per * 2, :]

    def merge(p):
        with jax.named_scope("waitd"):
            copy_d(p).wait_recv()
        comb[:, p] = stage_h[p, core] + recv_d[p]
        each(1, chips, lambda k: copy_h(k, p).start())

    @pl.loop(0, pairs)
    def _(p):
        step(p)
        copy_d(p).start()

        @pl.when(p >= LAG)
        def _():
            merge(p - LAG)

        @pl.when((p == pairs - TURN) & (core == 1))
        def _():
            for j in range(own):
                with jax.named_scope("waitc"):
                    got_c(j).wait()
                mine_t[j] = stage_c[j * nt + my_t] + jnp.sum(recv_c[j, 1:group], axis=0)
                each(1, chips, lambda k: copy_t(j, k).start())

    for p in range(pairs - LAG, pairs):
        merge(p)

    @pl.when(core == 1)
    def _():
        rows = BINS // LANES
        small[1].wait()
        xs = []
        for j in range(own):
            with jax.named_scope("waitt"):
                got_t(j).wait()
            xs.append(mine_t[j] + jnp.sum(recv_t[j, 1:chips], axis=0))
        x = jnp.concatenate(xs, axis=0)
        top = jnp.floor(x * (1.0 / 65536.0))
        x = x - top * 65536.0
        mid = jnp.floor(x * (1.0 / 256.0))
        low = x - mid * 256.0
        digits = [v.astype(BF16) for v in (low, mid, top)]
        size = own * rows
        r0, r1 = iota((size, size), 0), iota((size, size), 1)
        upper = flag(iota((LANES, LANES), 0) <= iota((LANES, LANES), 1))
        before = flag((r0 // rows == r1 // rows) & (r1 < r0))

        def value(parts):
            return parts[0] + parts[1] * 256.0 + parts[2] * 65536.0

        within = value([jnp.dot(v, upper, preferred_element_type=F32) for v in digits])
        ahead = value([jnp.dot(before, v, preferred_element_type=F32) for v in digits])
        cum = within + jnp.sum(ahead, axis=1, keepdims=True)
        for j in range(own):
            goal = retain[j * nt + my_t].astype(F32)
            less = jnp.where(cum[j * rows:(j + 1) * rows] < goal, 1.0, 0.0)
            all_g[my_t, j] = jnp.sum(less, axis=0, keepdims=True)
        each(1, group, lambda k: copy_g(k).start())
        with jax.named_scope("waitg"):
            got_g(nt - 1).wait()

    @pl.when(core == 0)
    def _():
        small[1].wait()
        with jax.named_scope("waitg"):
            got_g(nt).wait()

    counts = jnp.concatenate([all_g[p % nt, p // nt] for p in range(pairs)], axis=0)
    if pairs < LANES:
        counts = jnp.concatenate([counts, jnp.zeros((LANES - pairs, LANES), F32)], axis=0)
    ones = jnp.ones((8, LANES), BF16)
    found = lax.dot_general(ones, counts.astype(BF16), NT, preferred_element_type=F32)
    thresh[...] = found.astype(jnp.int32)

    with jax.named_scope("waith"):
        got_h().wait()
    for p in range(pairs):
        acc = comb[chip, p] + jnp.sum(recv_h[1:chips, p], axis=0)
        for h in range(heads):
            for j in range(per):
                at = (h * per + j) * 2
                out[p, h, :, j * lanes:(j + 1) * lanes] = acc[at:at + 2, :]

    for p in range(pairs):
        k, copy = copy_c(p)
        pl.when(k > 0)(copy.wait_send)

    @pl.when(core == 1)
    def _():
        for j in range(own):
            each(1, chips, lambda k: copy_t(j, k).wait_send())
        each(1, group, lambda k: copy_g(k).wait_send())

    each(0, pairs, lambda p: copy_d(p).wait_send())
    whole = comb.at[pl.ds(0, chips - 1)]
    pltpu.make_async_copy(whole, whole, hs).wait()


def hand_over(hist, thresh, out, threshold):
    out[...] = hist[...]
    threshold[...] = thresh[0, :threshold.shape[0]]


def solution(mesh):
    n, nt = mesh.shape["seq"], mesh.shape["tensor"]

    def per_device(key_states, value_states, bin_index, retain_count):
        pairs, heads, toks = bin_index.shape
        span = BINS // n
        lanes = min(LANES, span)
        per = span // lanes
        group, chips = 2 * nt, n // 2
        own = pairs // nt
        rows = BINS // LANES
        block = (heads * per * 2, lanes)
        vmem = pltpu.VMEM
        dma = pltpu.SemaphoreType.DMA
        args = [
            pltpu.with_memory_space_constraint(x, pltpu.HBM)
            for x in (key_states, value_states, bin_index, retain_count)
        ]
        hist, thresh = pl.pallas_call(
            functools.partial(kernel, n, nt),
            out_shape=(
                jax.ShapeDtypeStruct((pairs, heads, 2, span), F32),
                jax.ShapeDtypeStruct((8, LANES), jnp.int32),
            ),
            in_specs=[pl.BlockSpec(memory_space=pltpu.HBM)] * 4,
            out_specs=(pl.BlockSpec(memory_space=vmem), pl.BlockSpec(memory_space=vmem)),
            scratch_shapes=[
                vmem((pairs, 2) + key_states.shape[1:], BF16),
                vmem(bin_index.shape, jnp.int32),
                pltpu.SMEM(retain_count.shape, jnp.int32),
                vmem((pairs, rows, LANES), F32),
                vmem((own, group, rows, LANES), F32),
                vmem((own, rows, LANES), F32),
                vmem((own, chips, rows, LANES), F32),
                vmem((nt, own, 1, LANES), F32),
                vmem((pairs, 2, chips) + block, F32),
                vmem((pairs, chips) + block, F32),
                vmem((chips, pairs) + block, F32),
                vmem((chips, pairs) + block, F32),
                dma((2, pairs)), dma((2,)),
                dma, dma((own,)), dma, dma((own,)),
                dma, dma, dma, dma((pairs,)),
                dma, dma,
            ],
            compiler_params=pltpu.CompilerParams(
                collective_id=0, has_side_effects=True, vmem_limit_bytes=32 * 2**20
            ),
        )(*args)
        return pl.pallas_call(
            hand_over,
            out_shape=(
                jax.ShapeDtypeStruct(hist.shape, F32),
                jax.ShapeDtypeStruct(retain_count.shape, jnp.int32),
            ),
            in_specs=[pl.BlockSpec(memory_space=vmem)] * 2,
            out_specs=(pl.BlockSpec(memory_space=vmem), pl.BlockSpec(memory_space=vmem)),
            compiler_params=pltpu.CompilerParams(vmem_limit_bytes=4 * 2**20),
        )(hist, thresh)

    in_specs = (
        P(None, None, "seq", "tensor"),
        P(None, None, "seq", "tensor"),
        P(None, "tensor", "seq"),
        P(),
    )
    out_specs = (P(None, "tensor", None, "seq"), P())
    return jax.shard_map(
        per_device, mesh=mesh, in_specs=in_specs, out_specs=out_specs, check_vma=False
    )
```

```python
import functools

import jax
import jax.numpy as jnp
from jax import lax
from jax.experimental import pallas as pl
from jax.experimental.pallas import tpu as pltpu
from jax.sharding import PartitionSpec as P

BINS = 4096
LANES = 128
HALF = 64
LAG = 2
EARLY = 1
TURN = 5
RELAY = 4
MESH = pl.DeviceIdType.MESH
NT = (((1,), (1,)), ((), ()))
F32 = jnp.float32
BF16 = jnp.bfloat16


def iota(shape, dim):
    return lax.broadcasted_iota(jnp.int32, shape, dim)


def each(lo, hi, body):
    if hi - lo <= 8:
        for k in range(lo, hi):
            body(k)
    else:

        @pl.loop(lo, hi)
        def _(k):
            body(k)


def flag(cond):
    return jnp.where(cond, jnp.ones((), BF16), jnp.zeros((), BF16))


def narrow(row):
    return row.astype(F32).astype(BF16)


def kernel(
    n, nt, key_hbm, value_hbm, bins_hbm, retain_hbm, out, thresh,
    kv, bins, retain, stage_c, recv_c, mine_t, recv_t, all_g, stage_h, recv_d, comb, recv_h, recv_r,
    in_sem, bin_sem, cs, cr, ts, tr, gs, gr, ds, dr, hs, hr, rr,
):
    pairs, heads, toks = bins.shape
    width = kv.shape[4] // heads
    lanes = stage_h.shape[4]
    his = BINS // lanes
    per = his // n
    group, chips = 2 * nt, n // 2
    own = pairs // nt
    me = lax.axis_index("seq")
    my_t = lax.axis_index("tensor")
    chip, core = me // 2, me % 2
    spot = my_t * 2 + core

    def in_plane(k):
        g = lax.rem(spot + k, group)
        return {"seq": chip * 2 + g % 2, "tensor": g // 2}

    def in_line(k):
        z = lax.rem(chip + k, chips)
        return z, {"seq": z * 2 + core}

    relay = recv_r.shape[0] if chips == 4 else 0

    def mirror(z, r):
        return jnp.where(r < chips // 2, z, chips - 1 - z)

    spoke = mirror(chip, chip)
    inner = spoke == 1

    def nth(i):
        return lax.rem(i + jnp.where(inner, relay, 0), pairs) if relay else i

    def slot(z):
        if relay:
            return jnp.maximum(mirror(chip, z) - 1, 0)
        return lax.rem(z - chip + chips, chips) - 1

    barrier = pltpu.get_barrier_semaphore()

    def greet(device):
        pl.semaphore_signal(barrier, inc=1, device_id=device, device_id_type=MESH)

    each(1, group, lambda k: greet(in_plane(k)))
    each(1, chips, lambda k: greet(in_line(k)[1]))

    def load(p, i):
        return pltpu.make_async_copy((key_hbm, value_hbm)[i].at[p], kv.at[p, i], in_sem.at[i, p])

    small = (
        pltpu.make_async_copy(bins_hbm, bins, bin_sem.at[0]),
        pltpu.make_async_copy(retain_hbm, retain, bin_sem.at[1]),
    )
    small[0].start()
    for p in range(EARLY):
        load(nth(p), 0).start()
        load(nth(p), 1).start()
    with jax.named_scope("binwait"):
        small[0].wait()
    for p in range(EARLY, pairs):
        load(nth(p), 0).start()
        load(nth(p), 1).start()
    small[1].start()

    shift = HALF.bit_length() - 1
    code = iota((HALF, toks), 0)
    order = narrow(jnp.where(code < HALF // 2, code * 2, code * 2 - HALF + 1))
    code = narrow(code)
    total = jnp.zeros((BINS // LANES, LANES), F32)
    for p in range(pairs):
        grid = None
        for h in range(heads):
            row = bins[p, pl.ds(h, 1), :]
            lo = flag(code == narrow(row & (HALF - 1)))
            hi = flag(order == narrow(row >> shift))
            part = lax.dot_general(hi, lo, NT, preferred_element_type=F32)
            grid = part if grid is None else grid + part
        total += jnp.concatenate([grid[:HALF // 2], grid[HALF // 2:]], axis=1)
        stage_c[p] = total

    with jax.named_scope("barrier"):
        pl.semaphore_wait(barrier, group - 1 + chips - 1)

    def copy_c(p):
        k = lax.rem(p % nt * 2 + 1 - spot + group, group)
        return k, pltpu.make_async_remote_copy(
            src_ref=stage_c.at[p], dst_ref=recv_c.at[p // nt, k], send_sem=cs, recv_sem=cr.at[p // nt],
            device_id={"seq": chip * 2 + 1, "tensor": p % nt}, device_id_type=MESH)

    def got_c(j):
        part = recv_c.at[j, pl.ds(1, group - 1)]
        return pltpu.make_async_copy(part, part, cr.at[j])

    def copy_t(j, k):
        return pltpu.make_async_remote_copy(
            src_ref=mine_t.at[j], dst_ref=recv_t.at[j, k], send_sem=ts, recv_sem=tr.at[j],
            device_id=in_line(k)[1], device_id_type=MESH)

    def got_t(j):
        part = recv_t.at[j, pl.ds(1, chips - 1)]
        return pltpu.make_async_copy(part, part, tr.at[j])

    def copy_g(k):
        return pltpu.make_async_remote_copy(
            src_ref=all_g.at[my_t], dst_ref=all_g.at[my_t], send_sem=gs, recv_sem=gr,
            device_id=in_plane(k), device_id_type=MESH)

    def got_g(m):
        part = all_g.at[pl.ds(0, m)]
        return pltpu.make_async_copy(part, part, gr)

    def copy_d(p):
        return pltpu.make_async_remote_copy(
            src_ref=stage_h.at[p, 1 - core], dst_ref=recv_d.at[p], send_sem=ds, recv_sem=dr.at[p],
            device_id={"seq": chip * 2 + 1 - core}, device_id_type=MESH)

    def copy_h(z, p):
        to = slot(z)
        return pltpu.make_async_remote_copy(
            src_ref=comb.at[z, p], dst_ref=recv_h.at[to, p], send_sem=hs, recv_sem=hr.at[to // 2 if relay else 0],
            device_id={"seq": z * 2 + core}, device_id_type=MESH)

    def copy_r(i, p):
        return pltpu.make_async_remote_copy(
            src_ref=comb.at[mirror(2 + i, chip), p], dst_ref=recv_r.at[p, i], send_sem=hs, recv_sem=rr.at[p],
            device_id={"seq": mirror(1, chip) * 2 + core}, device_id_type=MESH)

    def wait_h():
        if not relay:
            return pltpu.make_async_copy(recv_h, recv_h, hr.at[0]).wait()
        for i, part in enumerate((recv_h.at[pl.ds(0, 2)], recv_h.at[2, pl.ds(relay, pairs - relay)])):
            pltpu.make_async_copy(part, part, hr.at[i]).wait()

    for p in range(pairs):
        k, copy = copy_c(p)
        pl.when(k > 0)(copy.start)

    blk = LANES
    eye = flag(iota((width, width), 0) == iota((width, width), 1))

    def cosine(p, i, h):
        parts = []
        for t in range(0, toks, blk):
            a = kv[p, i, 0, t:t + blk, h * width:(h + 1) * width]
            b = kv[p, i, 1, t:t + blk, h * width:(h + 1) * width]
            if t // blk in (0, 1, 2, 3):
                a, b = a.T.astype(F32), b.T.astype(F32)
            else:
                both = jnp.concatenate([a, b], axis=0)
                turned = lax.dot_general(eye, both, NT, preferred_element_type=F32)
                a, b = turned[:, :blk], turned[:, blk:]
            ab, aa, bb = (jnp.sum(x, axis=0, keepdims=True) for x in (a * b, a * a, b * b))
            parts.append(ab * lax.rsqrt((aa + 1.0) * (bb + 1.0)))
        return jnp.concatenate(parts, axis=1)

    cut = lanes.bit_length() - 1
    odd = (iota((2 * his, toks), 0) & 1) == 1
    hi_of = narrow(iota((2 * his, toks), 0) >> 1)
    lo_of = narrow(iota((lanes, toks), 0))

    def step(p):
        with jax.named_scope("loadwait"):
            load(p, 0).wait()
            load(p, 1).wait()
        for h in range(heads):
            kc = cosine(p, 0, h)
            vc = cosine(p, 1, h)
            row = bins[p, pl.ds(h, 1), :]
            both = jnp.where(odd, vc, kc).astype(BF16)
            left = jnp.where(hi_of == narrow(row >> cut), both, jnp.zeros_like(both))
            right = flag(lo_of == narrow(row & (lanes - 1)))
            res = lax.dot_general(left, right, NT, preferred_element_type=F32)
            for o in range(n):
                stage_h[p, o % 2, o // 2, pl.ds(h * per * 2, per * 2), :] = res[o * per * 2:(o + 1) * per * 2, :]

    def merge(i):
        p = nth(i)
        with jax.named_scope("waitd"):
            copy_d(p).wait_recv()
        comb[:, p] = stage_h[p, core] + recv_d[p]
        if not relay:
            return each(1, chips, lambda k: copy_h(in_line(k)[0], p).start())

        @pl.when((p < relay) & jnp.logical_not(inner))
        def _():
            copy_r(0, p).start()
            copy_r(1, p).start()
            copy_h(mirror(1, chip), p).start()

        @pl.when((p < relay) & inner)
        def _():
            got = recv_r.at[p]
            with jax.named_scope("waitr"):
                pltpu.make_async_copy(got, got, rr.at[p]).wait()
            for i in range(2):
                comb[mirror(2 + i, chip), p] += recv_r[p, i]

        @pl.when((p >= relay) | inner)
        def _():
            each(1, chips, lambda k: copy_h(in_line(k)[0], p).start())

    @pl.loop(0, pairs)
    def _(i):
        p = nth(i)
        step(p)
        copy_d(p).start()

        @pl.when(i >= LAG)
        def _():
            merge(i - LAG)

        @pl.when((i == pairs - TURN) & (core == 1))
        def _():
            for j in range(own):
                with jax.named_scope("waitc"):
                    got_c(j).wait()
                mine_t[j] = stage_c[j * nt + my_t] + jnp.sum(recv_c[j, 1:group], axis=0)
                each(1, chips, lambda k: copy_t(j, k).start())

    for p in range(pairs - LAG, pairs):
        merge(p)

    @pl.when(core == 1)
    def _():
        rows = BINS // LANES
        small[1].wait()
        xs = []
        for j in range(own):
            with jax.named_scope("waitt"):
                got_t(j).wait()
            xs.append(mine_t[j] + jnp.sum(recv_t[j, 1:chips], axis=0))
        x = jnp.concatenate(xs, axis=0)
        top = jnp.floor(x * (1.0 / 65536.0))
        x = x - top * 65536.0
        mid = jnp.floor(x * (1.0 / 256.0))
        low = x - mid * 256.0
        digits = [v.astype(BF16) for v in (low, mid, top)]
        size = own * rows
        r0, r1 = iota((size, size), 0), iota((size, size), 1)
        upper = flag(iota((LANES, LANES), 0) <= iota((LANES, LANES), 1))
        before = flag((r0 // rows == r1 // rows) & (r1 < r0))

        def value(parts):
            return parts[0] + parts[1] * 256.0 + parts[2] * 65536.0

        within = value([jnp.dot(v, upper, preferred_element_type=F32) for v in digits])
        ahead = value([jnp.dot(before, v, preferred_element_type=F32) for v in digits])
        cum = within + jnp.sum(ahead, axis=1, keepdims=True)
        for j in range(own):
            goal = retain[j * nt + my_t].astype(F32)
            less = jnp.where(cum[j * rows:(j + 1) * rows] < goal, 1.0, 0.0)
            all_g[my_t, j] = jnp.sum(less, axis=0, keepdims=True)
        each(1, group, lambda k: copy_g(k).start())
        with jax.named_scope("waitg"):
            got_g(nt - 1).wait()

    @pl.when(core == 0)
    def _():
        small[1].wait()
        with jax.named_scope("waitg"):
            got_g(nt).wait()

    counts = jnp.concatenate([all_g[p % nt, p // nt] for p in range(pairs)], axis=0)
    if pairs < LANES:
        counts = jnp.concatenate([counts, jnp.zeros((LANES - pairs, LANES), F32)], axis=0)
    ones = jnp.ones((8, LANES), BF16)
    found = lax.dot_general(ones, counts.astype(BF16), NT, preferred_element_type=F32)
    thresh[...] = found.astype(jnp.int32)

    with jax.named_scope("waith"):
        wait_h()
    for p in range(pairs):
        acc = comb[chip, p] + jnp.sum(recv_h[:2 if p < relay else chips - 1, p], axis=0)
        for h in range(heads):
            for j in range(per):
                at = (h * per + j) * 2
                out[p, h, :, j * lanes:(j + 1) * lanes] = acc[at:at + 2, :]

    for p in range(pairs):
        k, copy = copy_c(p)
        pl.when(k > 0)(copy.wait_send)

    @pl.when(core == 1)
    def _():
        for j in range(own):
            each(1, chips, lambda k: copy_t(j, k).wait_send())
        each(1, group, lambda k: copy_g(k).wait_send())

    each(0, pairs, lambda p: copy_d(p).wait_send())
    whole = comb.at[pl.ds(0, chips - 1)]
    pltpu.make_async_copy(whole, whole, hs).wait()


def hand_over(hist, thresh, out, threshold):
    out[...] = hist[...]
    threshold[...] = thresh[0, :threshold.shape[0]]


def solution(mesh):
    n, nt = mesh.shape["seq"], mesh.shape["tensor"]

    def per_device(key_states, value_states, bin_index, retain_count):
        pairs, heads, toks = bin_index.shape
        span = BINS // n
        lanes = min(LANES, span)
        per = span // lanes
        group, chips = 2 * nt, n // 2
        own = pairs // nt
        rows = BINS // LANES
        block = (heads * per * 2, lanes)
        vmem = pltpu.VMEM
        dma = pltpu.SemaphoreType.DMA
        args = [
            pltpu.with_memory_space_constraint(x, pltpu.HBM)
            for x in (key_states, value_states, bin_index, retain_count)
        ]
        hist, thresh = pl.pallas_call(
            functools.partial(kernel, n, nt),
            out_shape=(
                jax.ShapeDtypeStruct((pairs, heads, 2, span), F32),
                jax.ShapeDtypeStruct((8, LANES), jnp.int32),
            ),
            in_specs=[pl.BlockSpec(memory_space=pltpu.HBM)] * 4,
            out_specs=(pl.BlockSpec(memory_space=vmem), pl.BlockSpec(memory_space=vmem)),
            scratch_shapes=[
                vmem((pairs, 2) + key_states.shape[1:], BF16),
                vmem(bin_index.shape, jnp.int32),
                pltpu.SMEM(retain_count.shape, jnp.int32),
                vmem((pairs, rows, LANES), F32),
                vmem((own, group, rows, LANES), F32),
                vmem((own, rows, LANES), F32),
                vmem((own, chips, rows, LANES), F32),
                vmem((nt, own, 1, LANES), F32),
                vmem((pairs, 2, chips) + block, F32),
                vmem((pairs, chips) + block, F32),
                vmem((chips, pairs) + block, F32),
                vmem((chips - 1, pairs) + block, F32),
                vmem((RELAY, 2) + block, F32),
                dma((2, pairs)), dma((2,)),
                dma, dma((own,)), dma, dma((own,)),
                dma, dma, dma, dma((pairs,)),
                dma, dma((2,)), dma((RELAY,)),
            ],
            compiler_params=pltpu.CompilerParams(
                collective_id=0, has_side_effects=True, vmem_limit_bytes=32 * 2**20
            ),
        )(*args)
        return pl.pallas_call(
            hand_over,
            out_shape=(
                jax.ShapeDtypeStruct(hist.shape, F32),
                jax.ShapeDtypeStruct(retain_count.shape, jnp.int32),
            ),
            in_specs=[pl.BlockSpec(memory_space=vmem)] * 2,
            out_specs=(pl.BlockSpec(memory_space=vmem), pl.BlockSpec(memory_space=vmem)),
            compiler_params=pltpu.CompilerParams(vmem_limit_bytes=4 * 2**20),
        )(hist, thresh)

    in_specs = (
        P(None, None, "seq", "tensor"),
        P(None, None, "seq", "tensor"),
        P(None, "tensor", "seq"),
        P(),
    )
    out_specs = (P(None, "tensor", None, "seq"), P())
    return jax.shard_map(
        per_device, mesh=mesh, in_specs=in_specs, out_specs=out_specs, check_vma=False
    )
```

```python
import functools

import jax
import jax.numpy as jnp
from jax import lax
from jax.experimental import pallas as pl
from jax.experimental.pallas import tpu as pltpu
from jax.sharding import PartitionSpec as P

BINS = 4096
LANES = 128
HALF = 64
LAG = 2
EARLY = 1
TURN = 4
RELAY = 4
ALONE = 1
MESH = pl.DeviceIdType.MESH
NT = (((1,), (1,)), ((), ()))
F32 = jnp.float32
BF16 = jnp.bfloat16


def iota(shape, dim):
    return lax.broadcasted_iota(jnp.int32, shape, dim)


def each(lo, hi, body):
    if hi - lo <= 8:
        for k in range(lo, hi):
            body(k)
    else:

        @pl.loop(lo, hi)
        def _(k):
            body(k)


def flag(cond):
    return jnp.where(cond, jnp.ones((), BF16), jnp.zeros((), BF16))


def narrow(row):
    return row.astype(F32).astype(BF16)


def kernel(
    n, nt, key_hbm, value_hbm, bins_hbm, retain_hbm, out, thresh,
    kv, bins, retain, stage_c, recv_c, mine_t, recv_t, all_g, stage_h, recv_d, comb, recv_h, recv_r,
    in_sem, bin_sem, cs, cr, ts, tr, gs, gr, ds, dr, hs, hr, rr,
):
    pairs, heads, toks = bins.shape
    width = kv.shape[4] // heads
    lanes = stage_h.shape[4]
    his = BINS // lanes
    per = his // n
    group, chips = 2 * nt, n // 2
    own = pairs // nt
    me = lax.axis_index("seq")
    my_t = lax.axis_index("tensor")
    chip, core = me // 2, me % 2
    spot = my_t * 2 + core

    def in_plane(k):
        g = lax.rem(spot + k, group)
        return {"seq": chip * 2 + g % 2, "tensor": g // 2}

    def in_line(k):
        z = lax.rem(chip + k, chips)
        return z, {"seq": z * 2 + core}

    relay = recv_r.shape[0] if chips == 4 else 0

    def mirror(z, r):
        return jnp.where(r < chips // 2, z, chips - 1 - z)

    spoke = mirror(chip, chip)
    inner = spoke == 1

    def nth(i):
        return lax.rem(i + jnp.where(inner, relay, 0), pairs) if relay else i

    def slot(z):
        if relay:
            return jnp.maximum(mirror(chip, z) - 1, 0)
        return lax.rem(z - chip + chips, chips) - 1

    barrier = pltpu.get_barrier_semaphore()

    def greet(device):
        pl.semaphore_signal(barrier, inc=1, device_id=device, device_id_type=MESH)

    each(1, group, lambda k: greet(in_plane(k)))
    each(1, chips, lambda k: greet(in_line(k)[1]))

    def load(p, i):
        return pltpu.make_async_copy((key_hbm, value_hbm)[i].at[p], kv.at[p, i], in_sem.at[p])

    small = (
        pltpu.make_async_copy(bins_hbm, bins, bin_sem.at[0]),
        pltpu.make_async_copy(retain_hbm, retain, bin_sem.at[1]),
    )
    small[0].start()
    for p in range(EARLY):
        load(nth(p), 0).start()
        load(nth(p), 1).start()
    with jax.named_scope("binwait"):
        small[0].wait()
    for p in range(EARLY, pairs):
        load(nth(p), 0).start()
        load(nth(p), 1).start()
    small[1].start()

    shift = HALF.bit_length() - 1
    code = iota((HALF, toks), 0)
    order = narrow(jnp.where(code < HALF // 2, code * 2, code * 2 - HALF + 1))
    code = narrow(code)
    total = jnp.zeros((BINS // LANES, LANES), F32)
    for p in range(pairs):
        grid = None
        for h in range(heads):
            row = bins[p, pl.ds(h, 1), :]
            lo = flag(code == narrow(row & (HALF - 1)))
            hi = flag(order == narrow(row >> shift))
            part = lax.dot_general(hi, lo, NT, preferred_element_type=F32)
            grid = part if grid is None else grid + part
        total += jnp.concatenate([grid[:HALF // 2], grid[HALF // 2:]], axis=1)
        stage_c[p] = total

    def copy_c(p):
        k = lax.rem(p % nt * 2 + 1 - spot + group, group)
        return k, pltpu.make_async_remote_copy(
            src_ref=stage_c.at[p], dst_ref=recv_c.at[p // nt, k], send_sem=cs, recv_sem=cr.at[p // nt],
            device_id={"seq": chip * 2 + 1, "tensor": p % nt}, device_id_type=MESH)

    def got_c(j):
        part = recv_c.at[j, pl.ds(1, group - 1)]
        return pltpu.make_async_copy(part, part, cr.at[j])

    def copy_t(j, k):
        return pltpu.make_async_remote_copy(
            src_ref=mine_t.at[j], dst_ref=recv_t.at[j, k], send_sem=ts, recv_sem=tr.at[j],
            device_id=in_line(k)[1], device_id_type=MESH)

    def got_t(j):
        part = recv_t.at[j, pl.ds(1, chips - 1)]
        return pltpu.make_async_copy(part, part, tr.at[j])

    def copy_g(k):
        return pltpu.make_async_remote_copy(
            src_ref=all_g.at[my_t], dst_ref=all_g.at[my_t], send_sem=gs, recv_sem=gr,
            device_id=in_plane(k), device_id_type=MESH)

    def got_g(m):
        part = all_g.at[pl.ds(0, m)]
        return pltpu.make_async_copy(part, part, gr)

    def copy_d(p):
        return pltpu.make_async_remote_copy(
            src_ref=stage_h.at[p, 1 - core], dst_ref=recv_d.at[p], send_sem=ds, recv_sem=dr.at[p],
            device_id={"seq": chip * 2 + 1 - core}, device_id_type=MESH)

    def copy_h(z, p):
        to = slot(z)
        return pltpu.make_async_remote_copy(
            src_ref=comb.at[z, p], dst_ref=recv_h.at[to, p], send_sem=hs, recv_sem=hr.at[to // 2 if relay else 0],
            device_id={"seq": z * 2 + core}, device_id_type=MESH)

    def copy_r(i, p):
        return pltpu.make_async_remote_copy(
            src_ref=comb.at[mirror(2 + i, chip), p], dst_ref=recv_r.at[p, i], send_sem=hs, recv_sem=rr.at[p],
            device_id={"seq": mirror(1, chip) * 2 + core}, device_id_type=MESH)

    def wait_h():
        if not relay:
            return pltpu.make_async_copy(recv_h, recv_h, hr.at[0]).wait()
        for i, part in enumerate((recv_h.at[pl.ds(0, 2)], recv_h.at[2, pl.ds(relay, pairs - relay)])):
            pltpu.make_async_copy(part, part, hr.at[i]).wait()

    blk = LANES
    eye = flag(iota((width, width), 0) == iota((width, width), 1))

    def cosine(p, i, h):
        parts = []
        for t in range(0, toks, blk):
            a = kv[p, i, 0, t:t + blk, h * width:(h + 1) * width]
            b = kv[p, i, 1, t:t + blk, h * width:(h + 1) * width]
            if t // blk in (0, 1, 2, 3):
                a, b = a.T.astype(F32), b.T.astype(F32)
            else:
                both = jnp.concatenate([a, b], axis=0)
                turned = lax.dot_general(eye, both, NT, preferred_element_type=F32)
                a, b = turned[:, :blk], turned[:, blk:]
            ab, aa, bb = (jnp.sum(x, axis=0, keepdims=True) for x in (a * b, a * a, b * b))
            parts.append(ab * lax.rsqrt((aa + 1.0) * (bb + 1.0)))
        return jnp.concatenate(parts, axis=1)

    cut = lanes.bit_length() - 1
    odd = (iota((2 * his, toks), 0) & 1) == 1
    hi_of = narrow(iota((2 * his, toks), 0) >> 1)
    lo_of = narrow(iota((lanes, toks), 0))

    def step(p):
        with jax.named_scope("loadwait"):
            pltpu.make_async_copy(kv.at[p], kv.at[p], in_sem.at[p]).wait()
        for h in range(heads):
            kc = cosine(p, 0, h)
            vc = cosine(p, 1, h)
            row = bins[p, pl.ds(h, 1), :]
            both = jnp.where(odd, vc, kc).astype(BF16)
            left = jnp.where(hi_of == narrow(row >> cut), both, jnp.zeros_like(both))
            right = flag(lo_of == narrow(row & (lanes - 1)))
            res = lax.dot_general(left, right, NT, preferred_element_type=F32)
            for o in range(n):
                stage_h[p, o % 2, o // 2, pl.ds(h * per * 2, per * 2), :] = res[o * per * 2:(o + 1) * per * 2, :]

    def merge(i):
        p = nth(i)
        with jax.named_scope("waitd"):
            copy_d(p).wait_recv()
        comb[:, p] = stage_h[p, core] + recv_d[p]
        if not relay:
            return each(1, chips, lambda k: copy_h(in_line(k)[0], p).start())

        @pl.when((p < relay) & jnp.logical_not(inner))
        def _():
            copy_r(0, p).start()
            copy_r(1, p).start()
            copy_h(mirror(1, chip), p).start()

        @pl.when((p < relay) & inner)
        def _():
            got = recv_r.at[p]
            with jax.named_scope("waitr"):
                pltpu.make_async_copy(got, got, rr.at[p]).wait()
            for i in range(2):
                comb[mirror(2 + i, chip), p] += recv_r[p, i]

        @pl.when((p >= relay) | inner)
        def _():
            each(1, chips, lambda k: copy_h(in_line(k)[0], p).start())

    @pl.loop(0, ALONE)
    def _(i):
        step(nth(i))

    with jax.named_scope("barrier"):
        pl.semaphore_wait(barrier, group - 1 + chips - 1)

    for p in range(pairs):
        k, copy = copy_c(p)
        pl.when(k > 0)(copy.start)

    for i in range(ALONE):
        copy_d(nth(i)).start()

    @pl.loop(ALONE, pairs)
    def _(i):
        p = nth(i)
        step(p)
        copy_d(p).start()

        @pl.when(i >= LAG)
        def _():
            merge(i - LAG)

        @pl.when((i == pairs - TURN) & (core == 1))
        def _():
            for j in range(own):
                with jax.named_scope("waitc"):
                    got_c(j).wait()
                mine_t[j] = stage_c[j * nt + my_t] + jnp.sum(recv_c[j, 1:group], axis=0)
                each(1, chips, lambda k: copy_t(j, k).start())

    for p in range(pairs - LAG, pairs):
        merge(p)

    @pl.when(core == 1)
    def _():
        rows = BINS // LANES
        small[1].wait()
        xs = []
        for j in range(own):
            with jax.named_scope("waitt"):
                got_t(j).wait()
            xs.append(mine_t[j] + jnp.sum(recv_t[j, 1:chips], axis=0))
        x = jnp.concatenate(xs, axis=0)
        top = jnp.floor(x * (1.0 / 65536.0))
        x = x - top * 65536.0
        mid = jnp.floor(x * (1.0 / 256.0))
        low = x - mid * 256.0
        digits = [v.astype(BF16) for v in (low, mid, top)]
        size = own * rows
        r0, r1 = iota((size, size), 0), iota((size, size), 1)
        upper = flag(iota((LANES, LANES), 0) <= iota((LANES, LANES), 1))
        before = flag((r0 // rows == r1 // rows) & (r1 < r0))

        def value(parts):
            return parts[0] + parts[1] * 256.0 + parts[2] * 65536.0

        within = value([jnp.dot(v, upper, preferred_element_type=F32) for v in digits])
        ahead = value([jnp.dot(before, v, preferred_element_type=F32) for v in digits])
        cum = within + jnp.sum(ahead, axis=1, keepdims=True)
        for j in range(own):
            goal = retain[j * nt + my_t].astype(F32)
            less = jnp.where(cum[j * rows:(j + 1) * rows] < goal, 1.0, 0.0)
            all_g[my_t, j] = jnp.sum(less, axis=0, keepdims=True)
        each(1, group, lambda k: copy_g(k).start())

    with jax.named_scope("waith"):
        wait_h()
    for p in range(pairs):
        acc = comb[chip, p] + jnp.sum(recv_h[:2 if p < relay else chips - 1, p], axis=0)
        for h in range(heads):
            for j in range(per):
                at = (h * per + j) * 2
                out[p, h, :, j * lanes:(j + 1) * lanes] = acc[at:at + 2, :]

    @pl.when(core == 1)
    def _():
        with jax.named_scope("waitg"):
            got_g(nt - 1).wait()

    @pl.when(core == 0)
    def _():
        small[1].wait()
        with jax.named_scope("waitg"):
            got_g(nt).wait()

    counts = jnp.concatenate([all_g[p % nt, p // nt] for p in range(pairs)], axis=0)
    if pairs < LANES:
        counts = jnp.concatenate([counts, jnp.zeros((LANES - pairs, LANES), F32)], axis=0)
    ones = jnp.ones((8, LANES), BF16)
    found = lax.dot_general(ones, counts.astype(BF16), NT, preferred_element_type=F32)
    thresh[...] = found.astype(jnp.int32)

    for p in range(pairs):
        k, copy = copy_c(p)
        pl.when(k > 0)(copy.wait_send)

    @pl.when(core == 1)
    def _():
        for j in range(own):
            each(1, chips, lambda k: copy_t(j, k).wait_send())
        each(1, group, lambda k: copy_g(k).wait_send())

    each(0, pairs, lambda p: copy_d(p).wait_send())
    whole = comb.at[pl.ds(0, chips - 1)]
    pltpu.make_async_copy(whole, whole, hs).wait()


def hand_over(hist, thresh, out, threshold):
    out[...] = hist[...]
    threshold[...] = thresh[0, :threshold.shape[0]]


def solution(mesh):
    n, nt = mesh.shape["seq"], mesh.shape["tensor"]

    def per_device(key_states, value_states, bin_index, retain_count):
        pairs, heads, toks = bin_index.shape
        span = BINS // n
        lanes = min(LANES, span)
        per = span // lanes
        group, chips = 2 * nt, n // 2
        own = pairs // nt
        rows = BINS // LANES
        block = (heads * per * 2, lanes)
        vmem = pltpu.VMEM
        dma = pltpu.SemaphoreType.DMA
        args = [
            pltpu.with_memory_space_constraint(x, pltpu.HBM)
            for x in (key_states, value_states, bin_index, retain_count)
        ]
        hist, thresh = pl.pallas_call(
            functools.partial(kernel, n, nt),
            out_shape=(
                jax.ShapeDtypeStruct((pairs, heads, 2, span), F32),
                jax.ShapeDtypeStruct((8, LANES), jnp.int32),
            ),
            in_specs=[pl.BlockSpec(memory_space=pltpu.HBM)] * 4,
            out_specs=(pl.BlockSpec(memory_space=vmem), pl.BlockSpec(memory_space=vmem)),
            scratch_shapes=[
                vmem((pairs, 2) + key_states.shape[1:], BF16),
                vmem(bin_index.shape, jnp.int32),
                pltpu.SMEM(retain_count.shape, jnp.int32),
                vmem((pairs, rows, LANES), F32),
                vmem((own, group, rows, LANES), F32),
                vmem((own, rows, LANES), F32),
                vmem((own, chips, rows, LANES), F32),
                vmem((nt, own, 1, LANES), F32),
                vmem((pairs, 2, chips) + block, F32),
                vmem((pairs, chips) + block, F32),
                vmem((chips, pairs) + block, F32),
                vmem((chips - 1, pairs) + block, F32),
                vmem((RELAY, 2) + block, F32),
                dma((pairs,)), dma((2,)),
                dma, dma((own,)), dma, dma((own,)),
                dma, dma, dma, dma((pairs,)),
                dma, dma((2,)), dma((RELAY,)),
            ],
            compiler_params=pltpu.CompilerParams(
                collective_id=0, has_side_effects=True, vmem_limit_bytes=32 * 2**20
            ),
        )(*args)
        return pl.pallas_call(
            hand_over,
            out_shape=(
                jax.ShapeDtypeStruct(hist.shape, F32),
                jax.ShapeDtypeStruct(retain_count.shape, jnp.int32),
            ),
            in_specs=[pl.BlockSpec(memory_space=vmem)] * 2,
            out_specs=(pl.BlockSpec(memory_space=vmem), pl.BlockSpec(memory_space=vmem)),
            compiler_params=pltpu.CompilerParams(vmem_limit_bytes=4 * 2**20),
        )(hist, thresh)

    in_specs = (
        P(None, None, "seq", "tensor"),
        P(None, None, "seq", "tensor"),
        P(None, "tensor", "seq"),
        P(),
    )
    out_specs = (P(None, "tensor", None, "seq"), P())
    return jax.shard_map(
        per_device, mesh=mesh, in_specs=in_specs, out_specs=out_specs, check_vma=False
    )
```
